32 devices in a mesh: stage: 1 (over z), data: 32 (over y, x, core).
Axes of the slice: x: 4, y: 4, z: 1, core: 2. Of those that a mesh axis runs over, the one named last changes fastest.
The devices are a block of a 4x4x8 slice.
Arguments:
- w_master: float32 [192, 1024, 512], P('stage', 'data')
- momentum: float32 [192, 1024, 512], P('stage', 'data')
- grad: bfloat16 [192, 1024, 512], P('stage', 'data')
Outputs:
- output 1: bfloat16 [192, 1024, 512], P('stage')
- output 2: float32 [192, 1024, 512], P('stage', 'data')
All inputs are finite; a program needn't handle non-finite values.
Results may differ from the reference program's by a relative error of at most 0.00787722.
Values are sent between devices in bfloat16 or wider.
A program may use at most 768 MiB of HBM per device.

```python
import math
import jax
import jax.numpy as jnp
from jax import lax

DATA_DEVS = 32
MATS_DEV = 6
D = 1024
FF_E = 512
NS_ITERS = 5

MOMENTUM = 0.95
LEARN_RATE = 0.02
WEIGHT_DECAY = 0.1
NORM_EPS = 1e-7
COEF_A = 3.4445
COEF_B = -4.7750
COEF_C = 2.0315
RMS_SCALE = 0.2 * math.sqrt(max(D, FF_E))


def setup_inputs(seed: int = 0, part: int = 0) -> dict:
    mat_count = MATS_DEV * DATA_DEVS
    key = jax.random.fold_in(jax.random.key(seed), part)
    keys = jax.random.split(key, 7)
    w_master = 0.02 * jax.random.normal(keys[0], (mat_count, D, FF_E), jnp.float32)
    left_fac = jax.random.normal(keys[1], (mat_count, D, 4), jnp.float32)
    right_fac = jax.random.normal(keys[2], (mat_count, 4, FF_E), jnp.float32)
    shared = 0.25 * jnp.einsum("mdr,mrf->mdf", left_fac, right_fac)
    row_scale = jax.random.uniform(keys[3], (mat_count, D, 1), jnp.float32, 0.5, 2.0)
    momentum = row_scale * (jax.random.normal(keys[4], (mat_count, D, FF_E), jnp.float32) + shared)
    grad_scale = jax.random.uniform(keys[5], (mat_count, D, 1), jnp.float32, 0.5, 2.0)
    grad = (grad_scale * jax.random.normal(keys[6], (mat_count, D, FF_E), jnp.float32)).astype(jnp.bfloat16)
    return {"w_master": w_master, "momentum": momentum, "grad": grad}


def newton_schulz(x_mat):
    for iteration in range(NS_ITERS):
        gram_mat = jnp.dot(x_mat, x_mat.T, preferred_element_type=jnp.float32).astype(jnp.bfloat16)
        square = jnp.dot(gram_mat, gram_mat, preferred_element_type=jnp.float32)
        poly_mat = (COEF_B * gram_mat.astype(jnp.float32) + COEF_C * square).astype(jnp.bfloat16)
        prod_mat = jnp.dot(poly_mat, x_mat, preferred_element_type=jnp.float32)
        x_mat = (COEF_A * x_mat.astype(jnp.float32) + prod_mat).astype(jnp.bfloat16)
    return x_mat


def orthogonalize(mom_one):
    frob_norm = jnp.sqrt(jnp.sum(mom_one * mom_one))
    x_mat = (mom_one.astype(jnp.bfloat16).astype(jnp.float32) / (frob_norm + NORM_EPS)).astype(jnp.bfloat16)
    if D > FF_E:
        x_mat = newton_schulz(x_mat.T).T
    else:
        x_mat = newton_schulz(x_mat)
    return x_mat.astype(jnp.float32) * RMS_SCALE


def reference(w_master, momentum, grad):
    mom_new = MOMENTUM * momentum + grad.astype(jnp.float32)

    def update_one(w_and_m):
        w_one, mom_one = w_and_m
        w_new = w_one - LEARN_RATE * (orthogonalize(mom_one) + WEIGHT_DECAY * w_one)
        return w_new.astype(jnp.bfloat16)

    params = lax.map(update_one, (w_master, mom_new))
    return params, mom_new
```

```python
import functools
import math
import jax
import jax.numpy as jnp
from jax import lax
from jax.experimental import pallas as pl
from jax.experimental.pallas import tpu as pltpu
from jax.sharding import PartitionSpec as P

NS_ITERS = 5
MOMENTUM = 0.95
LEARN_RATE = 0.02
WEIGHT_DECAY = 0.1
NORM_EPS = 1e-7
COEF_A = 3.4445
COEF_B = -4.7750
COEF_C = 2.0315


def momentum_kernel(*refs):
    mom_ref, grad_ref = refs[:2]
    new_ref, half_ref, sq_ref = refs[-3:]
    mom_new = MOMENTUM * mom_ref[...] + grad_ref[...].astype(jnp.float32)
    new_ref[...] = mom_new
    half_ref[...] = mom_new.astype(jnp.bfloat16)
    rows_sum = jnp.sum(mom_new * mom_new, axis=1)
    lanes = sq_ref.shape[-1]
    total = rows_sum[:, :lanes]
    for start in range(lanes, rows_sum.shape[1], lanes):
        total = total + rows_sum[:, start:start + lanes]
    sq_ref[:, 0] = total


def momentum_step(mom_rows, grad_rows, mom_new, group, first, count):
    mats, rows, cols = mom_rows.shape
    whole = pl.BlockSpec((group, rows, cols), lambda i: (first + i, 0, 0))
    in_specs, operands, aliases = [whole, whole], [mom_rows, grad_rows], {}
    if mom_new is not None:
        in_specs.append(pl.BlockSpec(memory_space=pl.ANY))
        operands.append(mom_new)
        aliases = {2: 0}
    return pl.pallas_call(
        momentum_kernel,
        grid=(count,),
        out_shape=(
            jax.ShapeDtypeStruct(mom_rows.shape, jnp.float32),
            jax.ShapeDtypeStruct((count * group, rows, cols), jnp.bfloat16),
            jax.ShapeDtypeStruct((count * group, 1, 128), jnp.float32),
        ),
        in_specs=in_specs,
        out_specs=(
            whole,
            pl.BlockSpec((group, rows, cols), lambda i: (i, 0, 0)),
            pl.BlockSpec((group, 1, 128), lambda i: (i, 0, 0)),
        ),
        input_output_aliases=aliases,
        cost_estimate=pl.CostEstimate(flops=10 * count * group * rows * cols, bytes_accessed=12 * count * group * rows * cols, transcendentals=0),
        name="momentum_step",
    )(*operands)


def ns_kernel(chunk, sq_ref, x_in_ref, x_out_ref):
    norm = jnp.sqrt(jnp.sum(sq_ref[:, chunk])) + NORM_EPS
    x_mat = (x_in_ref[...].astype(jnp.float32) / norm).astype(jnp.bfloat16)
    for iteration in range(NS_ITERS):
        gram_mat = lax.dot_general(x_mat, x_mat, (((0,), (0,)), ((), ())), preferred_element_type=jnp.float32)
        gram_mat = gram_mat.astype(jnp.bfloat16)
        square = jnp.dot(gram_mat, gram_mat, preferred_element_type=jnp.float32)
        poly_mat = (COEF_B * gram_mat.astype(jnp.float32) + COEF_C * square).astype(jnp.bfloat16)
        prod_mat = jnp.dot(x_mat, poly_mat, preferred_element_type=jnp.float32)
        x_mat = (COEF_A * x_mat.astype(jnp.float32) + prod_mat).astype(jnp.bfloat16)
    x_out_ref[...] = x_mat


def newton_schulz(owned, sq_all, chunk):
    return pl.pallas_call(
        functools.partial(ns_kernel, chunk),
        out_shape=jax.ShapeDtypeStruct(owned.shape, owned.dtype),
        in_specs=[pl.BlockSpec(memory_space=pltpu.VMEM)] * 2,
        out_specs=pl.BlockSpec(memory_space=pltpu.VMEM),
        cost_estimate=pl.CostEstimate(flops=7 * 10**9, bytes_accessed=4 * owned.size, transcendentals=0),
        name="newton_schulz",
    )(sq_all, owned)


def update_kernel(rms_scale, *refs):
    w_ref, ortho_ref, out_ref = refs[0], refs[1], refs[-1]
    w_rows = w_ref[...]
    ortho = ortho_ref[...].astype(jnp.float32) * rms_scale
    out_ref[...] = (w_rows - LEARN_RATE * (ortho + WEIGHT_DECAY * w_rows)).astype(jnp.bfloat16)


def weight_update(w_rows, ortho_rows, partial, chunk, slot, slots, rms_scale):
    mats, rows, cols = ortho_rows.shape
    half = mats // 2
    in_specs = [
        pl.BlockSpec((half, rows, cols), lambda i: (2 * chunk + i, 0, 0)),
        pl.BlockSpec((half, rows, cols), lambda i: (i, 0, 0)),
    ]
    operands, aliases = [w_rows, ortho_rows], {}
    if partial is not None:
        in_specs.append(pl.BlockSpec(memory_space=pl.ANY))
        operands.append(partial)
        aliases = {2: 0}
    return pl.pallas_call(
        functools.partial(update_kernel, rms_scale),
        grid=(2,),
        out_shape=jax.ShapeDtypeStruct((slots * mats, rows, cols), jnp.bfloat16),
        in_specs=in_specs,
        out_specs=pl.BlockSpec((half, rows, cols), lambda i: (2 * slot + i, 0, 0)),
        input_output_aliases=aliases,
        name="weight_update",
    )(*operands)


def place_kernel(*refs):
    gathered_ref, out_ref = refs[0], refs[-1]
    for dev in range(gathered_ref.shape[0]):
        out_ref[:, dev] = gathered_ref[dev]


def place(gathered, params, first_mat, shape, block):
    group, mats, rows, cols = gathered.shape
    steps = mats // block
    in_specs = [pl.BlockSpec((group, block, rows, cols), lambda i: (0, i, 0, 0))]
    operands = [gathered]
    aliases = {}
    if params is not None:
        in_specs.append(pl.BlockSpec(memory_space=pl.ANY))
        operands.append(params)
        aliases = {1: 0}
    return pl.pallas_call(
        place_kernel,
        grid=(steps,),
        out_shape=jax.ShapeDtypeStruct(shape, gathered.dtype),
        in_specs=in_specs,
        out_specs=pl.BlockSpec((block, group, rows, cols), lambda i: (first_mat // block + i, 0, 0, 0)),
        input_output_aliases=aliases,
        cost_estimate=pl.CostEstimate(flops=1 * 10**7, bytes_accessed=4 * gathered.size, transcendentals=0),
        name="place",
    )(*operands)


def after(value, *others):
    return lax.optimization_barrier((value, *others))[0] if others else value


def gather_plan(chunks):
    plan, first = [(0, 1)], 1
    while first < chunks:
        count = min(2, chunks - first)
        plan.append((first, count))
        first += count
    return plan


def solution(mesh):
    group = mesh.shape["data"]
    row_spec = P("stage", "data", None)
    full_spec = P("stage", None, None)

    def local_step(w_rows, mom_rows, grad_rows):
        mat_count, rows_dev, col_count = mom_rows.shape
        chunks = mat_count // group
        rms_scale = 0.2 * math.sqrt(max(rows_dev * group, col_count))
        mom_new, half_first, sq_first = momentum_step(mom_rows, grad_rows, None, group, 0, 1)
        sq_first = lax.all_to_all(sq_first, "data", 0, 0, tiled=True)
        shape = (mat_count, group, rows_dev, col_count)
        params, waiting, ahead = None, [], ()
        for first, count in gather_plan(chunks):
            w_new = None
            for chunk in range(first, first + count):
                if chunk == 0:
                    half, sq_all, sq_index = half_first, sq_first, 0
                else:
                    if chunk == 1:
                        mom_new = after(mom_new, *ahead)
                        mom_new, half_rest, sq_rest = momentum_step(mom_rows, grad_rows, mom_new, group, 1, chunks - 1)
                        sq_rest = sq_rest.reshape(chunks - 1, group, 128).transpose(1, 0, 2)
                        sq_rest = lax.all_to_all(sq_rest, "data", 0, 0, tiled=True)
                    half, sq_all, sq_index = half_rest[(chunk - 1) * group:chunk * group], sq_rest, chunk - 1
                half = after(half, *ahead)
                owned = lax.all_to_all(half, "data", 0, 0, tiled=True)
                x_mat = newton_schulz(owned.reshape(rows_dev * group, col_count), sq_all, sq_index)
                ortho_rows = lax.all_to_all(x_mat.reshape(group, rows_dev, col_count), "data", 0, 0, tiled=True)
                w_new = weight_update(w_rows, ortho_rows, w_new, chunk, chunk - first, count, rms_scale)
                ahead = (w_new,)
            waiting.append((lax.all_gather(w_new, "data", axis=0, tiled=False), first * group))
            if len(waiting) > 2:
                gathered, place_mat = waiting.pop(0)
                params = place(after(gathered, w_new), params, place_mat, shape, 2)
                ahead = (w_new, params)
        for gathered, place_mat in waiting:
            params = place(gathered, params, place_mat, shape, 2)
        return params.reshape(mat_count, group * rows_dev, col_count), mom_new

    return jax.shard_map(local_step, mesh=mesh, in_specs=(row_spec, row_spec, row_spec), out_specs=(full_spec, row_spec), check_vma=False)
```

```python
import functools
import math
import jax
import jax.numpy as jnp
from jax import lax
from jax.experimental import pallas as pl
from jax.experimental.pallas import tpu as pltpu
from jax.sharding import PartitionSpec as P

NS_ITERS = 5
MOMENTUM = 0.95
LEARN_RATE = 0.02
WEIGHT_DECAY = 0.1
NORM_EPS = 1e-7
COEF_A = 3.4445
COEF_B = -4.7750
COEF_C = 2.0315


def momentum_kernel(*refs):
    mom_ref, grad_ref = refs[:2]
    new_ref, half_ref, sq_ref = refs[-3:]
    mom_new = MOMENTUM * mom_ref[...] + grad_ref[...].astype(jnp.float32)
    new_ref[...] = mom_new
    half_ref[...] = mom_new.astype(jnp.bfloat16)
    rows_sum = jnp.sum(mom_new * mom_new, axis=1)
    lanes = sq_ref.shape[-1]
    total = rows_sum[:, :lanes]
    for start in range(lanes, rows_sum.shape[1], lanes):
        total = total + rows_sum[:, start:start + lanes]
    sq_ref[:, 0, 0] = total


def momentum_step(mom_rows, grad_rows, mom_new, group, first, count):
    mats, rows, cols = mom_rows.shape
    whole = pl.BlockSpec((group, rows, cols), lambda i: (first + i, 0, 0))
    in_specs, operands, aliases = [whole, whole], [mom_rows, grad_rows], {}
    if mom_new is not None:
        in_specs.append(pl.BlockSpec(memory_space=pl.ANY))
        operands.append(mom_new)
        aliases = {2: 0}
    return pl.pallas_call(
        momentum_kernel,
        grid=(count,),
        out_shape=(
            jax.ShapeDtypeStruct(mom_rows.shape, jnp.float32),
            jax.ShapeDtypeStruct((count * group, rows, cols), jnp.bfloat16),
            jax.ShapeDtypeStruct((group, count, 1, 128), jnp.float32),
        ),
        in_specs=in_specs,
        out_specs=(
            whole,
            pl.BlockSpec((group, rows, cols), lambda i: (i, 0, 0)),
            pl.BlockSpec((group, 1, 1, 128), lambda i: (0, i, 0, 0)),
        ),
        input_output_aliases=aliases,
        cost_estimate=pl.CostEstimate(flops=10 * count * group * rows * cols, bytes_accessed=12 * count * group * rows * cols, transcendentals=0),
        name="momentum_step",
    )(*operands)


def remote(src, dst, send_sem, recv_sem, device):
    return pltpu.make_async_remote_copy(
        src_ref=src, dst_ref=dst, send_sem=send_sem, recv_sem=recv_sem,
        device_id={"data": device}, device_id_type=pl.DeviceIdType.MESH)


def wait_bytes(ref, sem):
    pltpu.make_async_copy(ref, ref, sem).wait()


def send_blocks(group, source, landing, sems, lead):
    me = lax.axis_index("data")

    def send(step, carry):
        target = lax.rem(me + step, group)
        remote(source(target), landing.at[(*lead, me)], sems.at[(*lead, 0)], sems.at[(*lead, 1)], target).start()
        return carry

    lax.fori_loop(1, group, send, 0)


def exchange_kernel(group, first_mat, count, rms_scale, half_ref, sq_ref, w_ref, *refs):
    outs = refs[:-11]
    owned, ortho, x_buf, sq_buf, w_buf, in_sems, back_sems, sq_sems, own_sems, sq_own_sem, w_sem = refs[-11:]
    me = lax.axis_index("data")
    others = pl.ds(0, group - 1)
    rows, cols = owned.shape[-2:]
    load_w = pltpu.make_async_copy(w_ref.at[pl.ds(first_mat, count * group)], w_buf, w_sem)
    load_w.start()
    own_sq = pltpu.make_async_copy(sq_ref.at[me], sq_buf.at[me], sq_own_sem)
    own_sq.start()
    barrier = pltpu.get_barrier_semaphore()

    def greet(step, carry):
        pl.semaphore_signal(barrier, inc=1, device_id={"data": lax.rem(me + step, group)}, device_id_type=pl.DeviceIdType.MESH)
        return carry

    lax.fori_loop(1, group, greet, 0)
    pl.semaphore_wait(barrier, group - 1)

    send_blocks(group, lambda i: sq_ref.at[i], sq_buf, sq_sems, ())

    def own_block(chunk):
        return pltpu.make_async_copy(half_ref.at[chunk * group + me], owned.at[chunk, me], own_sems.at[chunk])

    def send_in(chunk, carry):
        send_blocks(group, lambda i: half_ref.at[chunk * group + i], owned, in_sems, (chunk,))
        own_block(chunk).start()
        return carry

    lax.fori_loop(0, count, send_in, 0)
    own_sq.wait()
    wait_bytes(sq_buf.at[others], sq_sems.at[1])

    def orthogonalize(chunk, carry):
        own_block(chunk).wait()
        wait_bytes(owned.at[chunk, others], in_sems.at[chunk, 1])
        norm = jnp.sqrt(jnp.sum(sq_buf[:, chunk])) + NORM_EPS
        x_mat = (owned[chunk].reshape(group * rows, cols).astype(jnp.float32) / norm).astype(jnp.bfloat16)
        for iteration in range(NS_ITERS):
            gram_mat = lax.dot_general(x_mat, x_mat, (((0,), (0,)), ((), ())), preferred_element_type=jnp.float32)
            gram_mat = gram_mat.astype(jnp.bfloat16)
            square = jnp.dot(gram_mat, gram_mat, preferred_element_type=jnp.float32)
            poly_mat = (COEF_B * gram_mat.astype(jnp.float32) + COEF_C * square).astype(jnp.bfloat16)
            prod_mat = jnp.dot(x_mat, poly_mat, preferred_element_type=jnp.float32)
            x_mat = (COEF_A * x_mat.astype(jnp.float32) + prod_mat).astype(jnp.bfloat16)
        x_buf[chunk] = x_mat.reshape(group, rows, cols)
        ortho[chunk, me] = x_buf[chunk, me]
        send_blocks(group, lambda i: x_buf.at[chunk, i], ortho, back_sems, (chunk,))
        return carry

    lax.fori_loop(0, count, orthogonalize, 0)

    load_w.wait()
    starts = [0]
    for out in outs:
        starts.append(starts[-1] + out.shape[0])
    for chunk in range(count):
        wait_bytes(ortho.at[chunk, others], back_sems.at[chunk, 1])
        for out, low, high in zip(outs, starts[:-1], starts[1:]):
            low_mat, high_mat = max(low, chunk * group), min(high, (chunk + 1) * group)

            def update(mat, carry, chunk=chunk, out=out, low=low):
                w_rows = w_buf[mat]
                o_rows = ortho[chunk, mat - chunk * group].astype(jnp.float32) * rms_scale
                out[mat - low] = (w_rows - LEARN_RATE * (o_rows + WEIGHT_DECAY * w_rows)).astype(jnp.bfloat16)
                return carry

            if low_mat < high_mat:
                lax.fori_loop(low_mat, high_mat, update, 0)

    wait_bytes(sq_buf.at[others], sq_sems.at[0])
    for chunk in range(count):
        wait_bytes(owned.at[chunk, others], in_sems.at[chunk, 0])
        wait_bytes(ortho.at[chunk, others], back_sems.at[chunk, 0])


def exchange(group, half, sq_part, w_rows, first_mat, splits, rms_scale, collective_id):
    mats, rows, cols = half.shape
    count = mats // group
    block = pltpu.VMEM((count, group, rows, cols), jnp.bfloat16)
    return pl.pallas_call(
        functools.partial(exchange_kernel, group, first_mat, count, rms_scale),
        out_shape=[jax.ShapeDtypeStruct((split, rows, cols), jnp.bfloat16) for split in splits],
        in_specs=[pl.BlockSpec(memory_space=pl.ANY)] * 3,
        out_specs=[pl.BlockSpec(memory_space=pltpu.VMEM)] * len(splits),
        scratch_shapes=[
            block,
            block,
            block,
            pltpu.VMEM(sq_part.shape, jnp.float32),
            pltpu.VMEM((mats, rows, cols), jnp.float32),
            pltpu.SemaphoreType.DMA((count, 2)),
            pltpu.SemaphoreType.DMA((count, 2)),
            pltpu.SemaphoreType.DMA((2,)),
            pltpu.SemaphoreType.DMA((count,)),
            pltpu.SemaphoreType.DMA,
            pltpu.SemaphoreType.DMA,
        ],
        compiler_params=pltpu.CompilerParams(collective_id=collective_id, has_side_effects=True, vmem_limit_bytes=56 * 2**20),
        cost_estimate=pl.CostEstimate(flops=count * 7 * 10**9, bytes_accessed=16 * half.size, transcendentals=0),
        name=f"exchange_{collective_id}",
    )(half, sq_part, w_rows)


def place_kernel(*refs):
    gathered_ref, out_ref = refs[0], refs[-1]
    for dev in range(gathered_ref.shape[0]):
        out_ref[:, dev] = gathered_ref[dev]


def place(gathered, params, first_mat, shape, block):
    group, mats, rows, cols = gathered.shape
    steps = mats // block
    in_specs = [pl.BlockSpec((group, block, rows, cols), lambda i: (0, i, 0, 0))]
    operands = [gathered]
    aliases = {}
    if params is not None:
        in_specs.append(pl.BlockSpec(memory_space=pl.ANY))
        operands.append(params)
        aliases = {1: 0}
    return pl.pallas_call(
        place_kernel,
        grid=(steps,),
        out_shape=jax.ShapeDtypeStruct(shape, gathered.dtype),
        in_specs=in_specs,
        out_specs=pl.BlockSpec((block, group, rows, cols), lambda i: (first_mat // block + i, 0, 0, 0)),
        input_output_aliases=aliases,
        cost_estimate=pl.CostEstimate(flops=1 * 10**7, bytes_accessed=4 * gathered.size, transcendentals=0),
        name="place",
    )(*operands)


def after(value, *others):
    return lax.optimization_barrier((value, *others))[0] if others else value


def stage_plan(chunks, group):
    first = min(2, chunks - 1)
    rest, last = (chunks - first) * group, 5 * group // 8
    return [(0, first, [first * group]), (first, chunks - first, [rest - last, last])]


def solution(mesh):
    group = mesh.shape["data"]
    row_spec = P("stage", "data", None)
    full_spec = P("stage", None, None)

    def local_step(w_rows, mom_rows, grad_rows):
        mat_count, rows_dev, col_count = mom_rows.shape
        chunks = mat_count // group
        rms_scale = 0.2 * math.sqrt(max(rows_dev * group, col_count))
        shape = (mat_count, group, rows_dev, col_count)
        mom_new, gathers, ahead = None, [], ()
        for number, (first, count, splits) in enumerate(stage_plan(chunks, group)):
            if mom_new is not None:
                mom_new = after(mom_new, *ahead)
            mom_new, half, sq_part = momentum_step(mom_rows, grad_rows, mom_new, group, first, count)
            ahead = exchange(group, half, sq_part, w_rows, first * group, splits, rms_scale, number)
            first_mat = first * group
            for w_new in ahead:
                gathers.append((lax.all_gather(w_new, "data", axis=0, tiled=False), first_mat))
                first_mat += w_new.shape[0]
        params = None
        for gathered, first_mat in gathers:
            params = place(gathered, params, first_mat, shape, 4)
        return params.reshape(mat_count, group * rows_dev, col_count), mom_new

    return jax.shard_map(local_step, mesh=mesh, in_specs=(row_spec, row_spec, row_spec), out_specs=(full_spec, row_spec), check_vma=False)
```

```python
import functools
import math
import jax
import jax.numpy as jnp
from jax import lax
from jax.experimental import pallas as pl
from jax.experimental.pallas import tpu as pltpu
from jax.sharding import PartitionSpec as P

NS_ITERS = 5
MOMENTUM = 0.95
LEARN_RATE = 0.02
WEIGHT_DECAY = 0.1
NORM_EPS = 1e-7
COEF_A = 3.4445
COEF_B = -4.7750
COEF_C = 2.0315


def momentum_kernel(mom_ref, grad_ref, new_ref):
    new_ref[...] = MOMENTUM * mom_ref[...] + grad_ref[...].astype(jnp.float32)


def momentum_step(mom_rows, grad_rows, steps):
    mats, rows, cols = mom_rows.shape
    spec = pl.BlockSpec((mats // steps, rows, cols), lambda i: (i, 0, 0))
    return pl.pallas_call(
        momentum_kernel,
        grid=(steps,),
        out_shape=jax.ShapeDtypeStruct(mom_rows.shape, jnp.float32),
        in_specs=[spec, spec],
        out_specs=spec,
        cost_estimate=pl.CostEstimate(flops=10 * mom_rows.size, bytes_accessed=10 * mom_rows.size, transcendentals=0),
        name="momentum_step",
    )(mom_rows, grad_rows)


def remote(src, dst, send_sem, recv_sem, device):
    return pltpu.make_async_remote_copy(
        src_ref=src, dst_ref=dst, send_sem=send_sem, recv_sem=recv_sem,
        device_id={"data": device}, device_id_type=pl.DeviceIdType.MESH)


def wait_bytes(ref, sem):
    pltpu.make_async_copy(ref, ref, sem).wait()


def send_blocks(group, source, landing, sems, lead):
    me = lax.axis_index("data")

    def send(step, carry):
        target = lax.rem(me + step, group)
        remote(source(target), landing.at[(*lead, me)], sems.at[(*lead, 0)], sems.at[(*lead, 1)], target).start()
        return carry

    lax.fori_loop(1, group, send, 0)


def exchange_kernel(group, first_mat, count, rms_scale, mom_ref, grad_ref, w_ref, *refs):
    outs = refs[:-14]
    (mom_buf, grad_buf, half_buf, sq_part, owned, ortho, x_buf, sq_buf, w_buf,
     load_sems, in_sems, back_sems, sq_sems, w_sem) = refs[-14:]
    me = lax.axis_index("data")
    others = pl.ds(0, group - 1)
    rows, cols = owned.shape[-2:]
    lanes = sq_buf.shape[-1]

    def loads(chunk):
        mats = pl.ds(first_mat + chunk * group, group)
        return (pltpu.make_async_copy(mom_ref.at[mats], mom_buf.at[chunk], load_sems.at[chunk, 0]),
                pltpu.make_async_copy(grad_ref.at[mats], grad_buf.at[chunk], load_sems.at[chunk, 1]))

    for chunk in range(count):
        for load in loads(chunk):
            load.start()
    load_w = pltpu.make_async_copy(w_ref.at[pl.ds(first_mat, count * group)], w_buf, w_sem)
    load_w.start()
    barrier = pltpu.get_barrier_semaphore()

    def greet(step, carry):
        pl.semaphore_signal(barrier, inc=1, device_id={"data": lax.rem(me + step, group)}, device_id_type=pl.DeviceIdType.MESH)
        return carry

    lax.fori_loop(1, group, greet, 0)

    def momentum(chunk):
        for load in loads(chunk):
            load.wait()

        def one(mat, carry):
            mom_new = MOMENTUM * mom_buf[chunk, mat] + grad_buf[chunk, mat].astype(jnp.float32)
            half_buf[chunk, mat] = mom_new.astype(jnp.bfloat16)
            rows_sum = jnp.sum(mom_new * mom_new, axis=0, keepdims=True)
            total = rows_sum[:, :lanes]
            for start in range(lanes, cols, lanes):
                total = total + rows_sum[:, start:start + lanes]
            sq_part[chunk, mat] = total
            return carry

        lax.fori_loop(0, group, one, 0, unroll=2)
        owned[chunk, me] = half_buf[chunk, me]
        sq_buf[chunk, me] = sq_part[chunk, me]

    def send_in(chunk):
        send_blocks(group, lambda i: sq_part.at[chunk, i], sq_buf, sq_sems, (chunk,))
        send_blocks(group, lambda i: half_buf.at[chunk, i], owned, in_sems, (chunk,))

    def later_chunk(chunk, carry):
        momentum(chunk)
        send_in(chunk)
        return carry

    momentum(0)
    pl.semaphore_wait(barrier, group - 1)
    send_in(0)
    lax.fori_loop(1, count, later_chunk, 0)

    def orthogonalize(chunk, carry):
        wait_bytes(sq_buf.at[chunk, others], sq_sems.at[chunk, 1])
        wait_bytes(owned.at[chunk, others], in_sems.at[chunk, 1])
        norm = jnp.sqrt(jnp.sum(sq_buf[chunk])) + NORM_EPS
        x_mat = (owned[chunk].reshape(group * rows, cols).astype(jnp.float32) / norm).astype(jnp.bfloat16)
        for iteration in range(NS_ITERS):
            gram_mat = lax.dot_general(x_mat, x_mat, (((0,), (0,)), ((), ())), preferred_element_type=jnp.float32)
            gram_mat = gram_mat.astype(jnp.bfloat16)
            square = jnp.dot(gram_mat, gram_mat, preferred_element_type=jnp.float32)
            poly_mat = (COEF_B * gram_mat.astype(jnp.float32) + COEF_C * square).astype(jnp.bfloat16)
            prod_mat = jnp.dot(x_mat, poly_mat, preferred_element_type=jnp.float32)
            x_mat = (COEF_A * x_mat.astype(jnp.float32) + prod_mat).astype(jnp.bfloat16)
        x_buf[chunk] = x_mat.reshape(group, rows, cols)
        ortho[chunk, me] = x_buf[chunk, me]
        send_blocks(group, lambda i: x_buf.at[chunk, i], ortho, back_sems, (chunk,))
        return carry

    lax.fori_loop(0, count, orthogonalize, 0)

    load_w.wait()
    starts = [0]
    for out in outs:
        starts.append(starts[-1] + out.shape[0])
    for chunk in range(count):
        wait_bytes(ortho.at[chunk, others], back_sems.at[chunk, 1])
        for out, low, high in zip(outs, starts[:-1], starts[1:]):
            low_mat, high_mat = max(low, chunk * group), min(high, (chunk + 1) * group)

            def update(mat, carry, chunk=chunk, out=out, low=low):
                w_rows = w_buf[mat]
                o_rows = ortho[chunk, mat - chunk * group].astype(jnp.float32) * rms_scale
                out[mat - low] = (w_rows - LEARN_RATE * (o_rows + WEIGHT_DECAY * w_rows)).astype(jnp.bfloat16)
                return carry

            if low_mat < high_mat:
                lax.fori_loop(low_mat, high_mat, update, 0)

    for chunk in range(count):
        wait_bytes(sq_buf.at[chunk, others], sq_sems.at[chunk, 0])
        wait_bytes(owned.at[chunk, others], in_sems.at[chunk, 0])
        wait_bytes(ortho.at[chunk, others], back_sems.at[chunk, 0])


def exchange(group, count, mom_rows, grad_rows, w_rows, first_mat, splits, rms_scale, collective_id):
    rows, cols = mom_rows.shape[1:]
    size = count * group * rows * cols
    block = pltpu.VMEM((count, group, rows, cols), jnp.bfloat16)
    wide_block = pltpu.VMEM((count, group, rows, cols), jnp.float32)
    sums = pltpu.VMEM((count, group, 1, 128), jnp.float32)
    return pl.pallas_call(
        functools.partial(exchange_kernel, group, first_mat, count, rms_scale),
        out_shape=[jax.ShapeDtypeStruct((split, rows, cols), jnp.bfloat16) for split in splits],
        in_specs=[pl.BlockSpec(memory_space=pl.ANY)] * 3,
        out_specs=[pl.BlockSpec(memory_space=pltpu.VMEM)] * len(splits),
        scratch_shapes=[
            wide_block,
            block,
            block,
            sums,
            block,
            block,
            block,
            sums,
            pltpu.VMEM((count * group, rows, cols), jnp.float32),
            pltpu.SemaphoreType.DMA((count, 2)),
            pltpu.SemaphoreType.DMA((count, 2)),
            pltpu.SemaphoreType.DMA((count, 2)),
            pltpu.SemaphoreType.DMA((count, 2)),
            pltpu.SemaphoreType.DMA,
        ],
        compiler_params=pltpu.CompilerParams(collective_id=collective_id, has_side_effects=True, vmem_limit_bytes=58 * 2**20),
        cost_estimate=pl.CostEstimate(flops=count * 7 * 10**9, bytes_accessed=16 * size, transcendentals=0),
        name=f"exchange_{collective_id}",
    )(mom_rows, grad_rows, w_rows)


def place_kernel(*refs):
    gathered_ref, out_ref = refs[0], refs[-1]
    for dev in range(gathered_ref.shape[0]):
        out_ref[:, dev] = gathered_ref[dev]


def place(gathered, params, first_mat, shape, block):
    group, mats, rows, cols = gathered.shape
    steps = mats // block
    in_specs = [pl.BlockSpec((group, block, rows, cols), lambda i: (0, i, 0, 0))]
    operands = [gathered]
    aliases = {}
    if params is not None:
        in_specs.append(pl.BlockSpec(memory_space=pl.ANY))
        operands.append(params)
        aliases = {1: 0}
    return pl.pallas_call(
        place_kernel,
        grid=(steps,),
        out_shape=jax.ShapeDtypeStruct(shape, gathered.dtype),
        in_specs=in_specs,
        out_specs=pl.BlockSpec((block, group, rows, cols), lambda i: (first_mat // block + i, 0, 0, 0)),
        input_output_aliases=aliases,
        cost_estimate=pl.CostEstimate(flops=1 * 10**7, bytes_accessed=4 * gathered.size, transcendentals=0),
        name="place",
    )(*operands)


def after(value, *others):
    return lax.optimization_barrier((value, *others))[0] if others else value


def stage_plan(chunks, group):
    first = min(2, chunks - 1)
    rest, last = (chunks - first) * group, 5 * group // 8
    return [(0, first, [first * group]), (first, chunks - first, [rest - last, last])]


def solution(mesh):
    group = mesh.shape["data"]
    row_spec = P("stage", "data", None)
    full_spec = P("stage", None, None)

    def local_step(w_rows, mom_rows, grad_rows):
        mat_count, rows_dev, col_count = mom_rows.shape
        chunks = mat_count // group
        rms_scale = 0.2 * math.sqrt(max(rows_dev * group, col_count))
        shape = (mat_count, group, rows_dev, col_count)
        gathers, ahead = [], ()
        for number, (first, count, splits) in enumerate(stage_plan(chunks, group)):
            w_ahead = after(w_rows, *ahead)
            ahead = exchange(group, count, mom_rows, grad_rows, w_ahead, first * group, splits, rms_scale, number)
            first_mat = first * group
            for w_new in ahead:
                gathers.append((lax.all_gather(w_new, "data", axis=0, tiled=False), first_mat))
                first_mat += w_new.shape[0]
        mom_new = momentum_step(after(mom_rows, *ahead), grad_rows, chunks)
        params = None
        for gathered, first_mat in gathers:
            params = place(gathered, params, first_mat, shape, 4)
        return params.reshape(mat_count, group * rows_dev, col_count), mom_new

    return jax.shard_map(local_step, mesh=mesh, in_specs=(row_spec, row_spec, row_spec), out_specs=(full_spec, row_spec), check_vma=False)
```

```python
import functools
import math
import jax
import jax.numpy as jnp
from jax import lax
from jax.experimental import pallas as pl
from jax.experimental.pallas import tpu as pltpu
from jax.sharding import PartitionSpec as P

NS_ITERS = 5
MOMENTUM = 0.95
LEARN_RATE = 0.02
WEIGHT_DECAY = 0.1
NORM_EPS = 1e-7
COEF_A = 3.4445
COEF_B = -4.7750
COEF_C = 2.0315


def momentum_kernel(mom_ref, grad_ref, new_ref):
    new_ref[...] = MOMENTUM * mom_ref[...] + grad_ref[...].astype(jnp.float32)


def momentum_step(mom_rows, grad_rows, steps):
    mats, rows, cols = mom_rows.shape
    spec = pl.BlockSpec((mats // steps, rows, cols), lambda i: (i, 0, 0))
    return pl.pallas_call(
        momentum_kernel,
        grid=(steps,),
        out_shape=jax.ShapeDtypeStruct(mom_rows.shape, jnp.float32),
        in_specs=[spec, spec],
        out_specs=spec,
        cost_estimate=pl.CostEstimate(flops=10 * mom_rows.size, bytes_accessed=10 * mom_rows.size, transcendentals=0),
        name="momentum_step",
    )(mom_rows, grad_rows)


def remote(src, dst, send_sem, recv_sem, device):
    return pltpu.make_async_remote_copy(
        src_ref=src, dst_ref=dst, send_sem=send_sem, recv_sem=recv_sem,
        device_id={"data": device}, device_id_type=pl.DeviceIdType.MESH)


def wait_bytes(ref, sem):
    pltpu.make_async_copy(ref, ref, sem).wait()


def send_blocks(group, source, landing, sems, lead):
    me = lax.axis_index("data")
    stride = 7 if group % 7 else 1

    def send(step, carry):
        target = lax.rem(me + stride * step, group)
        remote(source(target), landing.at[(*lead, me)], sems.at[(*lead, 0)], sems.at[(*lead, 1)], target).start()
        return carry

    lax.fori_loop(1, group, send, 0)


def exchange_kernel(group, first_mat, count, rms_scale, mom_ref, grad_ref, w_ref, *refs):
    outs = refs[:-14]
    (mom_buf, grad_buf, half_buf, sq_part, owned, ortho, x_buf, sq_buf, w_buf,
     load_sems, in_sems, back_sems, sq_sems, w_sem) = refs[-14:]
    me = lax.axis_index("data")
    others = pl.ds(0, group - 1)
    rows, cols = owned.shape[-2:]
    lanes = sq_buf.shape[-1]

    def loads(chunk):
        mats = pl.ds(first_mat + chunk * group, group)
        return (pltpu.make_async_copy(mom_ref.at[mats], mom_buf.at[chunk], load_sems.at[chunk, 0]),
                pltpu.make_async_copy(grad_ref.at[mats], grad_buf.at[chunk], load_sems.at[chunk, 1]))

    for chunk in range(count):
        for load in loads(chunk):
            load.start()
    load_w = pltpu.make_async_copy(w_ref.at[pl.ds(first_mat, count * group)], w_buf, w_sem)
    load_w.start()
    barrier = pltpu.get_barrier_semaphore()

    def greet(step, carry):
        pl.semaphore_signal(barrier, inc=1, device_id={"data": lax.rem(me + step, group)}, device_id_type=pl.DeviceIdType.MESH)
        return carry

    lax.fori_loop(1, group, greet, 0)

    def momentum(chunk):
        for load in loads(chunk):
            load.wait()

        def one(mat, carry):
            mom_new = MOMENTUM * mom_buf[chunk, mat] + grad_buf[chunk, mat].astype(jnp.float32)
            half_buf[chunk, mat] = mom_new.astype(jnp.bfloat16)
            rows_sum = jnp.sum(mom_new * mom_new, axis=0, keepdims=True)
            total = rows_sum[:, :lanes]
            for start in range(lanes, cols, lanes):
                total = total + rows_sum[:, start:start + lanes]
            sq_part[chunk, mat] = total
            return carry

        lax.fori_loop(0, group, one, 0, unroll=4)
        owned[chunk, me] = half_buf[chunk, me]
        sq_buf[chunk, me] = sq_part[chunk, me]

    def send_in(chunk):
        send_blocks(group, lambda i: sq_part.at[chunk, i], sq_buf, sq_sems, (chunk,))
        send_blocks(group, lambda i: half_buf.at[chunk, i], owned, in_sems, (chunk,))

    def later_chunk(chunk, carry):
        momentum(chunk)
        send_in(chunk)
        return carry

    momentum(0)
    pl.semaphore_wait(barrier, group - 1)
    send_in(0)
    lax.fori_loop(1, count, later_chunk, 0)

    def orthogonalize(chunk, carry):
        wait_bytes(sq_buf.at[chunk, others], sq_sems.at[chunk, 1])
        wait_bytes(owned.at[chunk, others], in_sems.at[chunk, 1])
        norm = jnp.sqrt(jnp.sum(sq_buf[chunk])) + NORM_EPS
        x_mat = (owned[chunk].reshape(group * rows, cols).astype(jnp.float32) / norm).astype(jnp.bfloat16)
        for iteration in range(NS_ITERS):
            gram_mat = lax.dot_general(x_mat, x_mat, (((0,), (0,)), ((), ())), preferred_element_type=jnp.float32)
            gram_mat = gram_mat.astype(jnp.bfloat16)
            square = jnp.dot(gram_mat, gram_mat, preferred_element_type=jnp.float32)
            poly_mat = (COEF_B * gram_mat.astype(jnp.float32) + COEF_C * square).astype(jnp.bfloat16)
            prod_mat = jnp.dot(x_mat, poly_mat, preferred_element_type=jnp.float32)
            x_mat = (COEF_A * x_mat.astype(jnp.float32) + prod_mat).astype(jnp.bfloat16)
        x_buf[chunk] = x_mat.reshape(group, rows, cols)
        ortho[chunk, me] = x_buf[chunk, me]
        send_blocks(group, lambda i: x_buf.at[chunk, i], ortho, back_sems, (chunk,))
        return carry

    lax.fori_loop(0, count, orthogonalize, 0)

    load_w.wait()
    starts = [0]
    for out in outs:
        starts.append(starts[-1] + out.shape[0])
    for chunk in range(count):
        wait_bytes(ortho.at[chunk, others], back_sems.at[chunk, 1])
        for out, low, high in zip(outs, starts[:-1], starts[1:]):
            low_mat, high_mat = max(low, chunk * group), min(high, (chunk + 1) * group)

            def update(mat, carry, chunk=chunk, out=out, low=low):
                w_rows = w_buf[mat]
                o_rows = ortho[chunk, mat - chunk * group].astype(jnp.float32) * rms_scale
                out[mat - low] = (w_rows - LEARN_RATE * (o_rows + WEIGHT_DECAY * w_rows)).astype(jnp.bfloat16)
                return carry

            if low_mat < high_mat:
                lax.fori_loop(low_mat, high_mat, update, 0, unroll=4)

    for chunk in range(count):
        wait_bytes(sq_buf.at[chunk, others], sq_sems.at[chunk, 0])
        wait_bytes(owned.at[chunk, others], in_sems.at[chunk, 0])
        wait_bytes(ortho.at[chunk, others], back_sems.at[chunk, 0])


def exchange(group, count, mom_rows, grad_rows, w_rows, first_mat, splits, rms_scale, collective_id):
    rows, cols = mom_rows.shape[1:]
    size = count * group * rows * cols
    block = pltpu.VMEM((count, group, rows, cols), jnp.bfloat16)
    wide_block = pltpu.VMEM((count, group, rows, cols), jnp.float32)
    sums = pltpu.VMEM((count, group, 1, 128), jnp.float32)
    return pl.pallas_call(
        functools.partial(exchange_kernel, group, first_mat, count, rms_scale),
        out_shape=[jax.ShapeDtypeStruct((split, rows, cols), jnp.bfloat16) for split in splits],
        in_specs=[pl.BlockSpec(memory_space=pl.ANY)] * 3,
        out_specs=[pl.BlockSpec(memory_space=pltpu.VMEM)] * len(splits),
        scratch_shapes=[
            wide_block,
            block,
            block,
            sums,
            block,
            block,
            block,
            sums,
            pltpu.VMEM((count * group, rows, cols), jnp.float32),
            pltpu.SemaphoreType.DMA((count, 2)),
            pltpu.SemaphoreType.DMA((count, 2)),
            pltpu.SemaphoreType.DMA((count, 2)),
            pltpu.SemaphoreType.DMA((count, 2)),
            pltpu.SemaphoreType.DMA,
        ],
        compiler_params=pltpu.CompilerParams(collective_id=collective_id, has_side_effects=True, vmem_limit_bytes=58 * 2**20),
        cost_estimate=pl.CostEstimate(flops=count * 7 * 10**9, bytes_accessed=16 * size, transcendentals=0),
        name=f"exchange_{collective_id}",
    )(mom_rows, grad_rows, w_rows)


def place_kernel(first_mat, block, lead, *refs):
    gathered_ref, out_ref, buf, read_sems, write_sems = refs[0], *refs[-4:]
    steps, slots = gathered_ref.shape[1] // block, buf.shape[0]

    def read(step):
        slot = lax.rem(step, slots)
        return pltpu.make_async_copy(gathered_ref.at[:, pl.ds(step * block, block)], buf.at[slot], read_sems.at[slot])

    def writes(step):
        slot = lax.rem(step, slots)
        mat = first_mat + step * block
        return [pltpu.make_async_copy(buf.at[slot, :, i], out_ref.at[mat + i], write_sems.at[slot]) for i in range(block)]

    def wait_writes(step):
        slot = lax.rem(step, slots)
        wait_bytes(buf.at[slot], write_sems.at[slot])

    for step in range(min(lead, steps)):
        read(step).start()

    def one(step, carry):
        read(step).wait()
        for write in writes(step):
            write.start()

        @pl.when(step + lead < steps)
        def _():
            @pl.when(step + lead >= slots)
            def _():
                wait_writes(step + lead - slots)

            read(step + lead).start()

        return carry

    lax.fori_loop(0, steps, one, 0)
    for step in range(max(0, steps - slots), steps):
        wait_writes(step)


def place(gathered, params, first_mat, shape, block, slots):
    group, mats, rows, cols = gathered.shape
    in_specs = [pl.BlockSpec(memory_space=pl.ANY)]
    operands = [gathered]
    aliases = {}
    if params is not None:
        in_specs.append(pl.BlockSpec(memory_space=pl.ANY))
        operands.append(params)
        aliases = {1: 0}
    return pl.pallas_call(
        functools.partial(place_kernel, first_mat, block, slots // 2),
        out_shape=jax.ShapeDtypeStruct(shape, gathered.dtype),
        in_specs=in_specs,
        out_specs=pl.BlockSpec(memory_space=pl.ANY),
        scratch_shapes=[
            pltpu.VMEM((slots, group, block, rows, cols), gathered.dtype),
            pltpu.SemaphoreType.DMA((slots,)),
            pltpu.SemaphoreType.DMA((slots,)),
        ],
        input_output_aliases=aliases,
        compiler_params=pltpu.CompilerParams(vmem_limit_bytes=40 * 2**20),
        cost_estimate=pl.CostEstimate(flops=1 * 10**7, bytes_accessed=4 * gathered.size, transcendentals=0),
        name="place",
    )(*operands)


def after(value, *others):
    return lax.optimization_barrier((value, *others))[0] if others else value


def stage_plan(chunks, group):
    first = min(2, chunks - 1)
    rest, last = (chunks - first) * group, 5 * group // 8
    return [(0, first, [first * group]), (first, chunks - first, [rest - last, last])]


def solution(mesh):
    group = mesh.shape["data"]
    row_spec = P("stage", "data", None)
    full_spec = P("stage", None, None)

    def local_step(w_rows, mom_rows, grad_rows):
        mat_count, rows_dev, col_count = mom_rows.shape
        chunks = mat_count // group
        rms_scale = 0.2 * math.sqrt(max(rows_dev * group, col_count))
        shape = (mat_count, group, rows_dev, col_count)
        gathers, ahead = [], ()
        for number, (first, count, splits) in enumerate(stage_plan(chunks, group)):
            w_ahead = after(w_rows, *ahead)
            ahead = exchange(group, count, mom_rows, grad_rows, w_ahead, first * group, splits, rms_scale, number)
            first_mat = first * group
            for w_new in ahead:
                gathers.append((lax.all_gather(w_new, "data", axis=0, tiled=False), first_mat))
                first_mat += w_new.shape[0]
        mom_new = momentum_step(after(mom_rows, *ahead), grad_rows, chunks)
        params = None
        for gathered, first_mat in gathers:
            params = place(gathered, params, first_mat, shape, 2, 12)
        return params.reshape(mat_count, group * rows_dev, col_count), mom_new

    return jax.shard_map(local_step, mesh=mesh, in_specs=(row_spec, row_spec, row_spec), out_specs=(full_spec, row_spec), check_vma=False)
```
